256 devices in a mesh: gx: 4 (over x), gy: 4 (over y), gz: 16 (over z, core).
Axes of the slice: x: 4, y: 4, z: 8, core: 2. Of those that a mesh axis runs over, the one named last changes fastest.
Arguments:
- densities: float32 [7, 512, 128, 512], P(None, 'gz', 'gy', 'gx'), may hold values from -6 to 6
- residuals: float32 [7, 512, 128, 512], P(None, 'gz', 'gy', 'gx'), may hold values from -320 to 320
Outputs:
- new_density: float32 [512, 128, 512], P('gz', 'gy', 'gx')
- weights: float32 [7], replicated
The draws below stay inside these ranges and needn't reach their ends.
All inputs are finite; a program needn't handle non-finite values.
Results may differ from the reference program's by a relative error of at most 0.000087.
Values sent between devices are 32-bit elements; how exact they have to be, the bound alone decides.
A program may use at most 64 MiB of HBM per device.

```python
import math
import jax
import jax.numpy as jnp
from jax import lax

HIST1 = 7
SWEEPS = 3
NX = 512
NY = 128
NZ = 512


def draw_residuals(key, part):
    keys = jax.random.split(jax.random.fold_in(key, 11), 4)
    base = jnp.clip(jax.random.normal(keys[0], (1, NZ, NY, NX), jnp.float32), -6.0, 6.0)
    zpos = jnp.arange(NZ, dtype=jnp.float32) / NZ
    rows = jnp.exp(jax.random.uniform(keys[3], (1, 1, NY, 1), jnp.float32, 0.0, math.log(3.0)))
    noise = 0.7 * jnp.clip(jax.random.normal(keys[1], (HIST1, NZ, NY, NX), jnp.float32), -6.0, 6.0)
    mixing = jax.random.uniform(keys[2], (HIST1, 1, 1, 1), jnp.float32, 0.5, 1.0)
    ramp = jnp.power(10.0, zpos)
    return (mixing * base + noise) * ramp.reshape(1, NZ, 1, 1) * rows


def levels(own_key, extent, pieces, low, top_value):
    loudness, own = 1.0, jax.random.fold_in(own_key, 6)
    for axis_at, blocks in pieces:
        heights = jnp.exp(jax.random.uniform(jax.random.fold_in(own, axis_at), (blocks,), jnp.float32, low / len(pieces), top_value / len(pieces)))
        loudness = loudness * jnp.repeat(heights, extent[axis_at] // blocks).reshape([-1 if axis == axis_at else 1 for axis in range(len(extent))])
    return loudness


def scatter_about(own_key, dims, spread, bound, shards=(), held_as=jnp.bfloat16):
    array = spread * jax.random.normal(own_key, dims, jnp.float32)
    if shards:
        array = array * levels(own_key, dims, shards, -0.22, 0.18)
    return jnp.clip(array, -bound, bound).astype(held_as)


def setup_inputs(seed: int = 0) -> dict:
    seeds = jax.random.split(jax.random.key(seed), 3)
    return {
        "densities": scatter_about(seeds[0], (HIST1, NZ, NY, NX), 1.0, 6.0, ((1, 16), (2, 4), (3, 4)), jnp.float32),
        "residuals": draw_residuals(jax.random.fold_in(seeds[2], 71), 0),
    }


shift_value = 0.15
mix_amount = 0.7

def sweep_weights():
    diag_value = 6.0 + shift_value
    upper = (shift_value + 12.0) / diag_value
    lower = upper / 3.0
    return [1.0 / ((upper + lower) / 2.0 + (upper - lower) / 2.0 * math.cos(math.pi * (2 * k - 1) / (2 * SWEEPS))) for k in range(1, SWEEPS + 1)]

def neighbours(field):
    total = jnp.roll(field, 1, 0) + jnp.roll(field, -1, 0)
    total = total + jnp.roll(field, 1, 1) + jnp.roll(field, -1, 1)
    return total + jnp.roll(field, 1, 2) + jnp.roll(field, -1, 2)

def reference(densities, residuals):
    flat = residuals.reshape(HIST1, -1)
    gram = jnp.dot(flat.astype(jnp.float32), flat.T.astype(jnp.float32), precision=lax.Precision.HIGHEST, preferred_element_type=jnp.float32)
    factor = jnp.linalg.cholesky(gram)
    ones_column = jnp.ones((HIST1, 1), jnp.float32)
    middle = lax.linalg.triangular_solve(factor, ones_column, left_side=True, lower=True)
    solved = lax.linalg.triangular_solve(factor, middle, left_side=True, lower=True, transpose_a=True)[:, 0]
    weights = solved / jnp.sum(solved)
    blended = jnp.tensordot(weights, densities, axes=1, precision=lax.Precision.HIGHEST)
    combined = jnp.tensordot(weights, residuals, axes=1, precision=lax.Precision.HIGHEST)
    diag_value = 6.0 + shift_value
    omegas = sweep_weights()
    rhs = 6.0 * combined - neighbours(combined)
    iterate = omegas[0] * rhs / diag_value
    for position in range(1, SWEEPS):
        iterate = iterate + omegas[position] * (rhs - diag_value * iterate + neighbours(iterate)) / diag_value
    return (blended + mix_amount * iterate, weights)
```

```python
import functools
import itertools
import math

import jax
import jax.numpy as jnp
from jax import lax
from jax.experimental import pallas as pl
from jax.experimental.pallas import tpu as pltpu
from jax.sharding import PartitionSpec as P

MESH = pl.DeviceIdType.MESH
HIST = 7
SWEEPS = 3
HALO = 3
SHIFT = 0.15
MIX = 0.7
DIAG = 6.0 + SHIFT
PAIRS = [(i, j) for i in range(HIST) for j in range(i + 1)]
ZR = 5
SLOT = 16


def sweep_weights():
    upper = (SHIFT + 12.0) / DIAG
    lower = upper / 3.0
    return [
        1.0
        / (
            (upper + lower) / 2.0
            + (upper - lower) / 2.0 * math.cos(math.pi * (2 * k - 1) / (2 * SWEEPS))
        )
        for k in range(1, SWEEPS + 1)
    ]


W1, W2, W3 = sweep_weights()
A2 = ((1.0 - W2) * W1 + W2) / DIAG
B2 = W2 * W1 / DIAG / DIAG
K1 = MIX * (1.0 - W3)
K2 = MIX * W3 / DIAG


def lanes(shape):
    return lax.broadcasted_iota(jnp.int32, shape, len(shape) - 1)


def pulay(total):
    gram = {}
    for k, (i, j) in enumerate(PAIRS):
        gram[i, j] = jnp.broadcast_to(total[:, k : k + 1], (8, 128))
    low, inv, mid = {}, [], []
    for j in range(HIST):
        pivot = gram[j, j]
        for k in range(j):
            pivot = pivot - low[j, k] * low[j, k]
        inv.append(lax.rsqrt(pivot))
        for i in range(j + 1, HIST):
            value = gram[i, j]
            for k in range(j):
                value = value - low[i, k] * low[j, k]
            low[i, j] = value * inv[j]
        value = 1.0
        for k in range(j):
            value = value - low[j, k] * mid[k]
        mid.append(value * inv[j])
    solved = [None] * HIST
    for j in reversed(range(HIST)):
        value = mid[j]
        for k in range(j + 1, HIST):
            value = value - low[k, j] * solved[k]
        solved[j] = value * inv[j]
    scale = 1.0 / functools.reduce(jnp.add, solved)
    return [value * scale for value in solved]


def exchange(sizes, dens, res, acc, from_left, from_right, own_left, own_right, weights,
             R, D, C, T1, T2, G1, G2, load_sem, dens_sem, bulk_send, bulk_recv,
             edge_send, edge_recv, gram_send, gram_recv):
    NX, NY, NZ = sizes
    nz, ny = res.shape[1], res.shape[2]
    ring = R.shape[2]
    gx, gy, gz = lax.axis_index("gx"), lax.axis_index("gy"), lax.axis_index("gz")

    def device(dx=0, dy=0, dz=0):
        return {
            "gx": lax.rem(gx + dx % NX, NX),
            "gy": lax.rem(gy + dy % NY, NY),
            "gz": lax.rem(gz + dz % NZ, NZ),
        }

    plane_peers = [device(dx=a, dy=b) for a, b in itertools.product(range(NX), range(NY)) if a or b]
    line_peers = [device(dz=c) for c in range(1, NZ)]
    corner_peers = [device(dy=b, dz=c) for b in (-1, 1) for c in (-1, 1)]
    barrier = pltpu.get_barrier_semaphore()
    greeted = plane_peers + line_peers + corner_peers
    for peer in greeted:
        pl.semaphore_signal(barrier, inc=1, device_id=peer, device_id_type=MESH)

    chunks = load_sem.shape[0]
    depth = nz // chunks
    loads = []
    for c in range(chunks):
        copy = pltpu.make_async_copy(
            res.at[:, pl.ds(c * depth, depth)],
            R.at[:, pl.ds(HALO + c * depth, depth), pl.ds(0, ny)],
            load_sem.at[c],
        )
        copy.start()
        loads.append(copy)
    dens_copy = pltpu.make_async_copy(dens, D, dens_sem)
    dens_copy.start()

    def plane_products(z, sums):
        sums = list(sums)
        for t in range(ny // 8):
            rows = [R[i, HALO + z, 8 * t : 8 * t + 8, :] for i in range(HIST)]
            for k, (i, j) in enumerate(PAIRS):
                sums[k] = sums[k] + rows[i] * rows[j]
        return tuple(sums)

    sums = tuple(jnp.zeros((8, 128), jnp.float32) for _ in PAIRS)
    for c in range(chunks):
        loads[c].wait()
        sums = lax.fori_loop(c * depth, (c + 1) * depth, plane_products, sums)
    lane = lanes((8, 128))
    partial = jnp.zeros((8, 128), jnp.float32)
    for k in range(len(PAIRS)):
        partial = jnp.where(lane == k, jnp.sum(sums[k], axis=1, keepdims=True), partial)
    row = jnp.sum(partial, axis=0, keepdims=True)

    pl.semaphore_wait(barrier, len(greeted))

    def share(buf, slot, value, peers, phase):
        buf[slot] = value
        for peer in peers:
            pltpu.make_async_remote_copy(
                buf.at[slot], buf.at[slot], gram_send.at[phase], gram_recv.at[phase],
                device_id=peer, device_id_type=MESH,
            ).start()
        return buf.at[pl.ds(0, len(peers))]

    def summed(buf, others, phase):
        pltpu.make_async_copy(others, others, gram_recv.at[phase]).wait()
        total = buf[0]
        for k in range(1, buf.shape[0]):
            total = total + buf[k]
        return total

    others1 = share(G1, gx * NY + gy, row, plane_peers, 0)

    main = pl.ds(HALO, nz)
    inner = pl.ds(0, ny)
    end_z = HALO + nz
    moves = [
        (res.at[:, pl.ds(0, 3)], R.at[:, pl.ds(end_z, 3), inner], device(dz=-1)),
        (res.at[:, pl.ds(nz - 3, 3)], R.at[:, pl.ds(0, 3), inner], device(dz=1)),
    ]
    for sy, sz in itertools.product((-1, 1), (-1, 1)):
        zs, zd = (0, end_z) if sz < 0 else (nz - 2, 1)
        ys, yd = (0, ny) if sy < 0 else (ny - 2, ring - 2)
        moves.append((
            res.at[:, pl.ds(zs, 2), pl.ds(ys, 2)],
            R.at[:, pl.ds(zd, 2), pl.ds(yd, 2)],
            device(dy=sy, dz=sz),
        ))
    moves += [
        (res.at[:, :, pl.ds(0, 3)], R.at[:, main, pl.ds(ny, 3)], device(dy=-1)),
        (res.at[:, :, pl.ds(ny - 3, 3)], R.at[:, main, pl.ds(ring - 3, 3)], device(dy=1)),
    ]
    bulk = [
        pltpu.make_async_remote_copy(
            src, dst, bulk_send.at[k], bulk_recv.at[k], device_id=peer, device_id_type=MESH
        )
        for k, (src, dst, peer) in enumerate(moves)
    ]
    for copy in bulk:
        copy.start()

    others2 = share(G2, gz, summed(G1, others1, 0), line_peers, 1)
    total = summed(G2, others2, 1)
    shares = pulay(total)
    for i in range(HIST):
        weights[i] = shares[i]
    shares = [weights[i] for i in range(HIST)]
    for copy in bulk:
        copy.wait_recv()

    tiles = ring // 8

    def combine(k):
        out = None
        for i in range(HIST):
            term = shares[i][None] * R[i, k].reshape(tiles, 8, 128)
            out = term if out is None else out + term
        return out.reshape(ring, 128)

    for k in (0, nz + 2 * HALO - 1):
        C[k] = combine(k)
    wide = lanes((ring, 128))

    def combine_pack(p, packs):
        value = combine(p + 1)
        C[p + 1] = value
        base = (p // ZR) * SLOT + lax.rem(p, ZR) * HALO
        here = (wide >= base) & (wide < base + HALO)
        left, right = packs
        left = jnp.where(here, pltpu.roll(value, base, 1), left)
        right = jnp.where(here, pltpu.roll(value, base + HALO, 1), right)
        return left, right

    empty = jnp.zeros((ring, 128), jnp.float32)
    left, right = lax.fori_loop(0, nz + 4, combine_pack, (empty, empty))
    own_left[...] = left
    own_right[...] = right
    edges = [
        pltpu.make_async_remote_copy(
            own_left, from_right, edge_send.at[0], edge_recv.at[0],
            device_id=device(dx=-1), device_id_type=MESH,
        ),
        pltpu.make_async_remote_copy(
            own_right, from_left, edge_send.at[1], edge_recv.at[1],
            device_id=device(dx=1), device_id_type=MESH,
        ),
    ]
    for copy in edges:
        copy.start()

    first, last = wide == 0, wide == 127

    def around(v):
        total = pltpu.roll(v, 1, 0) + pltpu.roll(v, ring - 1, 0)
        total = total + jnp.where(first, 0.0, pltpu.roll(v, 1, 1))
        return total + jnp.where(last, 0.0, pltpu.roll(v, 127, 1))

    def sweep1(k, _):
        v = C[k + 1]
        T1[k] = 6.0 * v - (C[k] + C[k + 2] + around(v))
        return 0

    def sweep2(k, _):
        v = T1[k + 1]
        T2[k] = A2 * v + B2 * (T1[k] + T1[k + 2] + around(v))
        return 0

    def sweep3(k, _):
        v = T2[k + 1]
        out = K1 * v + K2 * (T1[k + 2] + T2[k] + T2[k + 2] + around(v))
        out = out[:ny].reshape(ny // 8, 8, 128)
        for i in range(HIST):
            out = out + shares[i][None] * D[i, k].reshape(ny // 8, 8, 128)
        acc[k] = out.reshape(ny, 128)
        return 0

    lax.fori_loop(0, nz + 4, sweep1, 0)
    lax.fori_loop(0, nz + 2, sweep2, 0)
    dens_copy.wait()
    lax.fori_loop(0, nz, sweep3, 0)

    for copy in edges:
        copy.wait()
    for copy in bulk:
        copy.wait_send()
    for phase, others in enumerate((others1, others2)):
        pltpu.make_async_copy(others, others, gram_send.at[phase]).wait()


def finish(acc, from_left, from_right, own_left, own_right, weights, out, coeffs, buf, sem):
    nz, ny = acc.shape[0], acc.shape[1]
    ring = from_left.shape[0]
    wide = lanes((ring, 128))
    place = wide % SLOT
    inside = (place >= HALO) & (place < 3 * HALO)

    packs = (from_left[...], own_left[...], own_right[...], from_right[...])

    def spread(zr):
        value = jnp.zeros((ring, 128), jnp.float32)
        for q, pack in enumerate(packs):
            moved = pltpu.roll(pack, (HALO * (q - zr)) % 128, 1)
            value = jnp.where((place >= HALO * q) & (place < HALO * (q + 1)), moved, value)
        return value

    def nb(v):
        out = []
        for zr in range(ZR):
            before = v[zr - 1] if zr else pltpu.roll(v[ZR - 1], SLOT, 1)
            after = v[zr + 1] if zr < ZR - 1 else pltpu.roll(v[0], 128 - SLOT, 1)
            total = before + after
            total = total + pltpu.roll(v[zr], 1, 0) + pltpu.roll(v[zr], ring - 1, 0)
            out.append(total + pltpu.roll(v[zr], 1, 1) + pltpu.roll(v[zr], 127, 1))
        return out

    def relaxed(start, keep):
        n0 = nb(start)
        r = [keep(6.0 * v - n) for v, n in zip(start, n0)]
        n1 = nb(r)
        u = [keep(A2 * v + B2 * n) for v, n in zip(r, n1)]
        n2 = nb(u)
        return [K1 * v + K2 * (s + n) for v, s, n in zip(u, r, n2)]

    def clip(v):
        return jnp.where(inside, v, 0.0)

    whole = [spread(zr) for zr in range(ZR)]
    true = relaxed(whole, lambda v: v)
    closed = relaxed([clip(v) for v in whole], clip)
    change = [(a - b)[:ny] for a, b in zip(true, closed)]
    lane = lanes((ny, 128))
    near, far = lane < HALO, lane >= 128 - HALO
    chunks = sem.shape[0]
    copies = []
    for z in range(nz):
        zq, zr = divmod(z + 2, ZR)
        at_left = pltpu.roll(change[zr], (-(SLOT * zq + HALO)) % 128, 1)
        at_right = pltpu.roll(change[zr], (125 - (SLOT * zq + 2 * HALO)) % 128, 1)
        buf[z] = acc[z] + jnp.where(near, at_left, jnp.where(far, at_right, 0.0))
        depth = nz // chunks
        if z % depth == depth - 1:
            c = z // depth
            part = pl.ds(c * depth, depth)
            copy = pltpu.make_async_copy(buf.at[part], out.at[part], sem.at[c])
            copy.start()
            copies.append(copy)
    coeff_lane = lanes((1, 128))
    row = jnp.zeros((1, 128), jnp.float32)
    for i in range(HIST):
        row = jnp.where(coeff_lane == i, weights[i, 0:1, :], row)
    coeffs[...] = row[:, :HIST]
    for copy in copies:
        copy.wait()


def on_device(sizes, densities, residuals):
    _, nz, ny, nx = residuals.shape
    ring, deep = ny + 8, nz + 2 * HALO
    f32 = jnp.float32
    vmem, hbm = pl.BlockSpec(memory_space=pltpu.VMEM), pl.BlockSpec(memory_space=pltpu.HBM)
    edge = pltpu.VMEM((ring, nx), f32)
    NX, NY, NZ = sizes
    dma = pltpu.SemaphoreType.DMA
    middle = pl.pallas_call(
        functools.partial(exchange, sizes),
        out_shape=(
            pltpu.VMEM((nz, ny, nx), f32), edge, edge, edge, edge,
            pltpu.VMEM((HIST, 8, 128), f32),
        ),
        in_specs=[hbm, hbm],
        out_specs=(vmem,) * 6,
        scratch_shapes=[
            pltpu.VMEM((HIST, deep, ring, nx), f32),
            pltpu.VMEM((HIST, nz, ny, nx), f32),
            pltpu.VMEM((deep, ring, nx), f32),
            pltpu.VMEM((deep - 2, ring, nx), f32),
            pltpu.VMEM((deep - 4, ring, nx), f32),
            pltpu.VMEM((NX * NY, 1, 128), f32),
            pltpu.VMEM((NZ, 1, 128), f32),
            dma((8,)), dma(()), dma((8,)), dma((8,)), dma((2,)), dma((2,)), dma((2,)), dma((2,)),
        ],
        compiler_params=pltpu.CompilerParams(
            collective_id=0, has_side_effects=True, vmem_limit_bytes=60 << 20
        ),
    )(densities, residuals)
    density, coeffs = pl.pallas_call(
        finish,
        out_shape=(
            jax.ShapeDtypeStruct((nz, ny, nx), f32),
            jax.ShapeDtypeStruct((1, HIST), f32),
        ),
        in_specs=[vmem] * 6,
        out_specs=(hbm, vmem),
        scratch_shapes=[pltpu.VMEM((nz, ny, nx), f32), dma((4,))],
        compiler_params=pltpu.CompilerParams(vmem_limit_bytes=16 << 20),
    )(*middle)
    return density, coeffs.reshape(HIST)


def solution(mesh):
    sizes = tuple(mesh.shape[a] for a in ("gx", "gy", "gz"))
    spec = P(None, "gz", "gy", "gx")
    return jax.shard_map(
        functools.partial(on_device, sizes),
        mesh=mesh,
        in_specs=(spec, spec),
        out_specs=(P("gz", "gy", "gx"), P()),
        check_vma=False,
    )
```

```python
import functools
import itertools
import math

import jax
import jax.numpy as jnp
from jax import lax
from jax.experimental import pallas as pl
from jax.experimental.pallas import tpu as pltpu
from jax.sharding import PartitionSpec as P

MESH = pl.DeviceIdType.MESH
HIST = 7
SWEEPS = 3
HALO = 3
SHIFT = 0.15
MIX = 0.7
DIAG = 6.0 + SHIFT
PAIRS = [(i, j) for i in range(HIST) for j in range(i + 1)]
ZR = 5
SLOT = 16


def sweep_weights():
    upper = (SHIFT + 12.0) / DIAG
    lower = upper / 3.0
    return [
        1.0
        / (
            (upper + lower) / 2.0
            + (upper - lower) / 2.0 * math.cos(math.pi * (2 * k - 1) / (2 * SWEEPS))
        )
        for k in range(1, SWEEPS + 1)
    ]


W1, W2, W3 = sweep_weights()
A2 = ((1.0 - W2) * W1 + W2) / DIAG
B2 = W2 * W1 / DIAG / DIAG
K1 = MIX * (1.0 - W3)
K2 = MIX * W3 / DIAG


def unrolled(count, step, body, init=None):
    def turn(q, carry):
        for j in range(step):
            carry = body(q * step + j, carry)
        return carry

    return lax.fori_loop(0, count // step, turn, init)


def lanes(shape):
    return lax.broadcasted_iota(jnp.int32, shape, len(shape) - 1)


def pulay(total):
    gram = {}
    for k, (i, j) in enumerate(PAIRS):
        gram[i, j] = jnp.broadcast_to(total[:, k : k + 1], (8, 128))
    low, inv, mid = {}, [], []
    for j in range(HIST):
        pivot = gram[j, j]
        for k in range(j):
            pivot = pivot - low[j, k] * low[j, k]
        inv.append(lax.rsqrt(pivot))
        for i in range(j + 1, HIST):
            value = gram[i, j]
            for k in range(j):
                value = value - low[i, k] * low[j, k]
            low[i, j] = value * inv[j]
        value = 1.0
        for k in range(j):
            value = value - low[j, k] * mid[k]
        mid.append(value * inv[j])
    solved = [None] * HIST
    for j in reversed(range(HIST)):
        value = mid[j]
        for k in range(j + 1, HIST):
            value = value - low[k, j] * solved[k]
        solved[j] = value * inv[j]
    scale = 1.0 / functools.reduce(jnp.add, solved)
    return [value * scale for value in solved]


def spread(packs):
    ring = next(pack.shape[0] for pack in packs if pack is not None)
    place = lanes((ring, 128)) % SLOT
    strips = []
    for zr in range(ZR):
        value = jnp.zeros((ring, 128), jnp.float32)
        for q, pack in enumerate(packs):
            if pack is not None:
                moved = pltpu.roll(pack, (HALO * (q - zr)) % 128, 1)
                value = jnp.where((place >= HALO * q) & (place < HALO * (q + 1)), moved, value)
        strips.append(value)
    return strips


def relaxed(start, closed=False):
    ring = start[0].shape[0]
    place = lanes((ring, 128)) % SLOT
    inside = (place >= HALO) & (place < 3 * HALO)

    def keep(v):
        return jnp.where(inside, v, 0.0) if closed else v

    def nb(v):
        out = []
        for zr in range(ZR):
            before = v[zr - 1] if zr else pltpu.roll(v[ZR - 1], SLOT, 1)
            after = v[zr + 1] if zr < ZR - 1 else pltpu.roll(v[0], 128 - SLOT, 1)
            total = before + after
            total = total + pltpu.roll(v[zr], 1, 0) + pltpu.roll(v[zr], ring - 1, 0)
            out.append(total + pltpu.roll(v[zr], 1, 1) + pltpu.roll(v[zr], 127, 1))
        return out

    r = [keep(6.0 * v - n) for v, n in zip(start, nb(start))]
    u = [keep(A2 * v + B2 * n) for v, n in zip(r, nb(r))]
    return [K1 * v + K2 * (s + n) for v, s, n in zip(u, r, nb(u))]


def exchange(sizes, dens, res, acc, from_left, from_right, strip, weights,
             R, D, C, T1, T2, G1, G2, packs, own_left, own_right,
             load_sem, dens_sem, bulk_send, bulk_recv,
             edge_send, edge_recv, gram_send, gram_recv, entered):
    NX, NY, NZ = sizes
    chips = NZ // 2
    nz, ny = res.shape[1], res.shape[2]
    ring = R.shape[2]
    gx, gy, gz = lax.axis_index("gx"), lax.axis_index("gy"), lax.axis_index("gz")

    def device(dx=0, dy=0, dz=0):
        return {
            "gx": lax.rem(gx + dx % NX, NX),
            "gy": lax.rem(gy + dy % NY, NY),
            "gz": lax.rem(gz + dz % NZ, NZ),
        }

    chip, core = gz // 2, lax.rem(gz, 2)

    def in_plane(dx, dy, other):
        to = device(dx=dx, dy=dy)
        if other:
            to["gz"] = 2 * chip + (1 - core)
        return to

    def along(step):
        to = lax.rem(chip + step, chips)
        return dict(device(), gz=2 * to + core), to > chip

    def hops(step):
        sizes_here = (NX, NY, 2) if len(step) == 3 else (chips,)
        return -sum(min(v, n - v) for v, n in zip(step, sizes_here))

    steps = sorted(itertools.product(range(NX), range(NY), range(2)), key=hops)
    plane_peers = [in_plane(*step) for step in steps if any(step)]
    line_peers = [along(*step) for step in sorted([(k,) for k in range(1, chips)], key=hops)]
    across = 2 * core - 1
    next_peers = [
        dict(device(dy=dy), gz=lax.rem(gz + across + NZ, NZ)) for dy in (-1, 0, 1)
    ]
    bottom, top = gz == 0, gz == NZ - 1
    barrier = pltpu.get_barrier_semaphore()

    def greet(semaphore, peer):
        pl.semaphore_signal(semaphore, inc=1, device_id=peer, device_id_type=MESH)

    def wait(semaphore, amount):
        pl.when(amount > 0)(functools.partial(pl.semaphore_wait, semaphore, amount))

    chunks = load_sem.shape[0]
    depth = nz // chunks
    loads = []
    for c in range(chunks):
        copy = pltpu.make_async_copy(
            res.at[:, pl.ds(c * depth, depth)],
            R.at[:, pl.ds(HALO + c * depth, depth), pl.ds(0, ny)],
            load_sem.at[c],
        )
        copy.start()
        loads.append(copy)
    dens_copy = pltpu.make_async_copy(dens, D, dens_sem)
    dens_copy.start()

    for peer, above in line_peers:
        pl.when(above)(functools.partial(greet, barrier, peer))
    for peer in plane_peers:
        greet(barrier, peer)

    @pl.when(jnp.logical_not(top))
    def _():
        for peer in next_peers:
            greet(barrier, peer)

    main = pl.ds(HALO, nz)
    inner = pl.ds(0, ny)
    end_z = HALO + nz
    moves = [
        (res.at[:, :, pl.ds(0, 3)], R.at[:, main, pl.ds(ny, 3)], device(dy=-1)),
        (res.at[:, :, pl.ds(ny - 3, 3)], R.at[:, main, pl.ds(ring - 3, 3)], device(dy=1)),
        (res.at[:, pl.ds(0, 3)], R.at[:, pl.ds(end_z, 3), inner], device(dz=-1)),
        (res.at[:, pl.ds(nz - 3, 3)], R.at[:, pl.ds(0, 3), inner], device(dz=1)),
    ]
    for sy, sz in itertools.product((-1, 1), (-1, 1)):
        zs, zd = (0, end_z) if sz < 0 else (nz - 2, 1)
        ys, yd = (0, ny) if sy < 0 else (ny - 2, ring - 2)
        moves.append((
            res.at[:, pl.ds(zs, 2), pl.ds(ys, 2)],
            R.at[:, pl.ds(zd, 2), pl.ds(yd, 2)],
            device(dy=sy, dz=sz),
        ))
    bulk = [
        pltpu.make_async_remote_copy(
            src, dst, bulk_send.at[k], bulk_recv.at[k], device_id=peer, device_id_type=MESH
        )
        for k, (src, dst, peer) in enumerate(moves)
    ]
    def plane_products(z, sums):
        sums = list(sums)
        for t in range(ny // 8):
            rows = [R[i, HALO + z, 8 * t : 8 * t + 8, :] for i in range(HIST)]
            for k, (i, j) in enumerate(PAIRS):
                sums[k] = sums[k] + rows[i] * rows[j]
        return tuple(sums)

    sums = tuple(jnp.zeros((8, 128), jnp.float32) for _ in PAIRS)
    for c in range(chunks):
        loads[c].wait()
        sums = lax.fori_loop(c * depth, (c + 1) * depth, plane_products, sums)
    lane = lanes((8, 128))
    partial = jnp.zeros((8, 128), jnp.float32)
    for k in range(len(PAIRS)):
        partial = jnp.where(lane == k, jnp.sum(sums[k], axis=1, keepdims=True), partial)
    row = jnp.sum(partial, axis=0, keepdims=True)

    def share(buf, slot, value, peers, phase):
        buf[slot] = value
        for peer in peers:
            pltpu.make_async_remote_copy(
                buf.at[slot], buf.at[slot], gram_send.at[phase], gram_recv.at[phase],
                device_id=peer, device_id_type=MESH,
            ).start()
        return buf.at[pl.ds(0, len(peers))]

    def summed(buf, others, phase):
        pltpu.make_async_copy(others, others, gram_recv.at[phase]).wait()
        total = buf[0]
        for k in range(1, buf.shape[0]):
            total = total + buf[k]
        return total

    few = len(next_peers)
    pl.semaphore_wait(barrier, len(plane_peers) + chip + few - few * bottom.astype(jnp.int32))
    others1 = share(G1, (gx * NY + gy) * 2 + core, row, plane_peers, 0)
    for peer, above in line_peers:
        pl.when(jnp.logical_not(above))(functools.partial(greet, entered.at[1], peer))

    @pl.when(top)
    def _():
        for peer in next_peers:
            greet(entered.at[0], peer)

    over = [bottom if k in (2, 4, 6) else None for k in range(len(bulk))]
    for copy, late in zip(bulk, over):
        if late is None:
            copy.start()
        else:
            pl.when(jnp.logical_not(late))(copy.start)

    @pl.when(bottom)
    def _():
        pl.semaphore_wait(entered.at[0], few)
        for k in (2, 4, 6):
            bulk[k].start()

    plane_row = summed(G1, others1, 0)
    wait(entered.at[1], chips - 1 - chip)
    others2 = share(G2, chip, plane_row, [peer for peer, _ in line_peers], 1)

    def pack_rows(low, high, i, _):
        wide = lanes((high - low, 128))
        for v in range((ZR + 1) // 2):
            part = jnp.zeros((high - low, 128), jnp.float32)
            for zr in range(2 * v, min(2 * v + 2, ZR)):
                for p in range(zr, nz + 4, ZR):
                    base = (p // ZR) * SLOT + 2 * HALO * (zr - 2 * v)
                    here = (wide >= base) & (wide < base + 2 * HALO)
                    moved = pltpu.roll(R[i, p + 1, low:high], (base + HALO) % 128, 1)
                    part = jnp.where(here, moved, part)
            packs[i, v, low:high] = part

    for copy in bulk[2:4]:
        copy.wait_recv()
    lax.fori_loop(0, HIST, functools.partial(pack_rows, 0, ny), None)
    for copy in bulk[:2] + bulk[4:]:
        copy.wait_recv()
    for i in range(HIST):
        pack_rows(ny, ring, i, None)
    wide = lanes((ring, 128))

    total = summed(G2, others2, 1)
    shares = pulay(total)
    for i in range(HIST):
        weights[i] = shares[i]
    shares = [weights[i] for i in range(HIST)]
    tiles = ring // 8

    def weighted(entries):
        out = None
        for share_i, entry in zip(shares, entries):
            term = share_i[None] * entry.reshape(-1, 8, 128)
            out = term if out is None else out + term
        return out.reshape(-1, 128)

    parts = [weighted([packs[i, v] for i in range(HIST)]) for v in range((ZR + 1) // 2)]
    place = wide % SLOT
    for side, own in enumerate((own_right, own_left)):
        edge = jnp.zeros((ring, 128), jnp.float32)
        for zr in range(ZR):
            source = 2 * HALO * (zr % 2) + HALO * side
            moved = pltpu.roll(parts[zr // 2], (HALO * zr - source) % 128, 1)
            edge = jnp.where((place >= HALO * zr) & (place < HALO * (zr + 1)), moved, edge)
        own[...] = edge
    edges = [
        pltpu.make_async_remote_copy(
            own_left, from_right, edge_send.at[0], edge_recv.at[0],
            device_id=device(dx=-1), device_id_type=MESH,
        ),
        pltpu.make_async_remote_copy(
            own_right, from_left, edge_send.at[1], edge_recv.at[1],
            device_id=device(dx=1), device_id_type=MESH,
        ),
    ]
    for copy in edges:
        copy.start()

    def combine(k, _):
        C[k] = weighted([R[i, k] for i in range(HIST)])

    unrolled(nz + 2 * HALO, (nz + 2 * HALO) // 2, combine)

    first, last = wide == 0, wide == 127

    def around(v):
        total = pltpu.roll(v, 1, 0) + pltpu.roll(v, ring - 1, 0)
        total = total + jnp.where(first, 0.0, pltpu.roll(v, 1, 1))
        return total + jnp.where(last, 0.0, pltpu.roll(v, 127, 1))

    def sweep1(k, _):
        v = C[k + 1]
        T1[k] = 6.0 * v - (C[k] + C[k + 2] + around(v))

    def sweep2(k, _):
        v = T1[k + 1]
        T2[k] = A2 * v + B2 * (T1[k] + T1[k + 2] + around(v))

    def sweep3(k, _):
        v = T2[k + 1]
        out = K1 * v + K2 * (T1[k + 2] + T2[k] + T2[k + 2] + around(v))
        acc[k] = out[:ny] + weighted([D[i, k] for i in range(HIST)])

    unrolled(nz + 4, 18, sweep1)
    unrolled(nz + 2, (nz + 2) // 2, sweep2)
    dens_copy.wait()
    unrolled(nz, 16, sweep3)
    own = spread((None, own_left[...], own_right[...], None))
    for zr, (a, b) in enumerate(zip(relaxed(own), relaxed(own, True))):
        strip[zr] = (a - b)[:ny]

    for copy in edges:
        copy.wait()
    for copy in bulk:
        copy.wait_send()
    for phase, others in enumerate((others1, others2)):
        pltpu.make_async_copy(others, others, gram_send.at[phase]).wait()


def finish(acc, from_left, from_right, strip, weights, out, coeffs, buf, row_buf, sem, row_sem):
    nz, ny = acc.shape[0], acc.shape[1]
    coeff_lane = lanes((1, 128))
    row = jnp.zeros((1, 128), jnp.float32)
    for i in range(HIST):
        row = jnp.where(coeff_lane == i, weights[i, 0:1, :], row)
    row_buf[...] = row[:, :HIST]
    row_copy = pltpu.make_async_copy(row_buf, coeffs, row_sem)
    row_copy.start()

    outer = spread((from_left[...], None, None, from_right[...]))
    change = [v[:ny] + strip[zr] for zr, v in enumerate(relaxed(outer))]
    lane = lanes((ny, 128))
    near, far = lane < HALO, lane >= 128 - HALO
    chunks = sem.shape[0]
    copies = []
    for z in range(nz):
        zq, zr = divmod(z + 2, ZR)
        at_left = pltpu.roll(change[zr], (-(SLOT * zq + HALO)) % 128, 1)
        at_right = pltpu.roll(change[zr], (125 - (SLOT * zq + 2 * HALO)) % 128, 1)
        buf[z] = acc[z] + jnp.where(near, at_left, jnp.where(far, at_right, 0.0))
        depth = nz // chunks
        if z % depth == depth - 1:
            c = z // depth
            part = pl.ds(c * depth, depth)
            copy = pltpu.make_async_copy(buf.at[part], out.at[part], sem.at[c])
            copy.start()
            copies.append(copy)
    for copy in copies:
        copy.wait()
    row_copy.wait()


def on_device(sizes, densities, residuals):
    _, nz, ny, nx = residuals.shape
    ring, deep = ny + 8, nz + 2 * HALO
    f32 = jnp.float32
    vmem, hbm = pl.BlockSpec(memory_space=pltpu.VMEM), pl.BlockSpec(memory_space=pltpu.HBM)
    edge = pltpu.VMEM((ring, nx), f32)
    NX, NY, NZ = sizes
    dma = pltpu.SemaphoreType.DMA
    middle = pl.pallas_call(
        functools.partial(exchange, sizes),
        out_shape=(
            pltpu.VMEM((nz, ny, nx), f32), edge, edge,
            pltpu.VMEM((ZR, ny, nx), f32), pltpu.VMEM((HIST, 8, 128), f32),
        ),
        in_specs=[hbm, hbm],
        out_specs=(vmem,) * 5,
        scratch_shapes=[
            pltpu.VMEM((HIST, deep, ring, nx), f32),
            pltpu.VMEM((HIST, nz, ny, nx), f32),
            pltpu.VMEM((deep, ring, nx), f32),
            pltpu.VMEM((deep - 2, ring, nx), f32),
            pltpu.VMEM((deep - 4, ring, nx), f32),
            pltpu.VMEM((NX * NY * 2, 1, 128), f32),
            pltpu.VMEM((NZ // 2, 1, 128), f32),
            pltpu.VMEM((HIST, (ZR + 1) // 2, ring, nx), f32),
            edge, edge,
            dma((8,)), dma(()), dma((8,)), dma((8,)), dma((2,)), dma((2,)), dma((2,)), dma((2,)),
            pltpu.SemaphoreType.REGULAR((2,)),
        ],
        compiler_params=pltpu.CompilerParams(
            collective_id=0, has_side_effects=True, vmem_limit_bytes=60 << 20
        ),
    )(densities, residuals)
    density, coeffs = pl.pallas_call(
        finish,
        out_shape=(
            jax.ShapeDtypeStruct((nz, ny, nx), f32),
            jax.ShapeDtypeStruct((1, HIST), f32),
        ),
        in_specs=[vmem] * 5,
        out_specs=(hbm, hbm),
        scratch_shapes=[
            pltpu.VMEM((nz, ny, nx), f32), pltpu.VMEM((1, HIST), f32), dma((4,)), dma(()),
        ],
        compiler_params=pltpu.CompilerParams(vmem_limit_bytes=16 << 20),
    )(*middle)
    return density, coeffs.reshape(HIST)


def solution(mesh):
    sizes = tuple(mesh.shape[a] for a in ("gx", "gy", "gz"))
    spec = P(None, "gz", "gy", "gx")
    return jax.shard_map(
        functools.partial(on_device, sizes),
        mesh=mesh,
        in_specs=(spec, spec),
        out_specs=(P("gz", "gy", "gx"), P()),
        check_vma=False,
    )
```

```python
import functools
import itertools
import math

import jax
import jax.numpy as jnp
from jax import lax
from jax.experimental import pallas as pl
from jax.experimental.pallas import tpu as pltpu
from jax.sharding import PartitionSpec as P

MESH = pl.DeviceIdType.MESH
HIST = 7
SWEEPS = 3
HALO = 3
SHIFT = 0.15
MIX = 0.7
DIAG = 6.0 + SHIFT
PAIRS = [(i, j) for i in range(HIST) for j in range(i + 1)]
ZR = 5
SLOT = 16


def sweep_weights():
    upper = (SHIFT + 12.0) / DIAG
    lower = upper / 3.0
    return [
        1.0
        / (
            (upper + lower) / 2.0
            + (upper - lower) / 2.0 * math.cos(math.pi * (2 * k - 1) / (2 * SWEEPS))
        )
        for k in range(1, SWEEPS + 1)
    ]


W1, W2, W3 = sweep_weights()
A2 = ((1.0 - W2) * W1 + W2) / DIAG
B2 = W2 * W1 / DIAG / DIAG
K1 = MIX * (1.0 - W3)
K2 = MIX * W3 / DIAG


def unrolled(count, step, body, init=None):
    def turn(q, carry):
        for j in range(step):
            carry = body(q * step + j, carry)
        return carry

    return lax.fori_loop(0, count // step, turn, init)


def lanes(shape):
    return lax.broadcasted_iota(jnp.int32, shape, len(shape) - 1)


def pulay(total):
    gram = {}
    for k, (i, j) in enumerate(PAIRS):
        gram[i, j] = jnp.broadcast_to(total[:, k : k + 1], (8, 128))
    low, inv, mid = {}, [], []
    for j in range(HIST):
        pivot = gram[j, j]
        for k in range(j):
            pivot = pivot - low[j, k] * low[j, k]
        inv.append(lax.rsqrt(pivot))
        for i in range(j + 1, HIST):
            value = gram[i, j]
            for k in range(j):
                value = value - low[i, k] * low[j, k]
            low[i, j] = value * inv[j]
        value = 1.0
        for k in range(j):
            value = value - low[j, k] * mid[k]
        mid.append(value * inv[j])
    solved = [None] * HIST
    for j in reversed(range(HIST)):
        value = mid[j]
        for k in range(j + 1, HIST):
            value = value - low[k, j] * solved[k]
        solved[j] = value * inv[j]
    scale = 1.0 / functools.reduce(jnp.add, solved)
    return [value * scale for value in solved]


def spread(left, right):
    ring = left.shape[0]
    place = lanes((ring, 128)) % SLOT
    strips = []
    for zr in range(ZR):
        value = jnp.zeros((ring, 128), jnp.float32)
        for q, pack in ((0, left), (3, right)):
            moved = pltpu.roll(pack, (HALO * (q - zr)) % 128, 1)
            value = jnp.where((place >= HALO * q) & (place < HALO * (q + 1)), moved, value)
        strips.append(value)
    return strips


def relaxed(start):
    ring = start[0].shape[0]

    def nb(v):
        out = []
        for zr in range(ZR):
            before = v[zr - 1] if zr else pltpu.roll(v[ZR - 1], SLOT, 1)
            after = v[zr + 1] if zr < ZR - 1 else pltpu.roll(v[0], 128 - SLOT, 1)
            total = before + after
            total = total + pltpu.roll(v[zr], 1, 0) + pltpu.roll(v[zr], ring - 1, 0)
            out.append(total + pltpu.roll(v[zr], 1, 1) + pltpu.roll(v[zr], 127, 1))
        return out

    r = [6.0 * v - n for v, n in zip(start, nb(start))]
    u = [A2 * v + B2 * n for v, n in zip(r, nb(r))]
    return [K1 * v + K2 * (s + n) for v, s, n in zip(u, r, nb(u))]


def exchange(sizes, dens, res, acc, from_left, from_right, own_left, own_right, weights,
             R, D, C, T1, T2, G1, G2, packs,
             load_sem, dens_sem, bulk_send, bulk_recv,
             edge_send, edge_recv, gram_send, gram_recv, entered):
    NX, NY, NZ = sizes
    chips = NZ // 2
    nz, ny = res.shape[1], res.shape[2]
    ring = R.shape[2]
    gx, gy, gz = lax.axis_index("gx"), lax.axis_index("gy"), lax.axis_index("gz")

    def device(dx=0, dy=0, dz=0):
        return {
            "gx": lax.rem(gx + dx % NX, NX),
            "gy": lax.rem(gy + dy % NY, NY),
            "gz": lax.rem(gz + dz % NZ, NZ),
        }

    chip, core = gz // 2, lax.rem(gz, 2)

    def in_plane(dx, dy, other):
        to = device(dx=dx, dy=dy)
        if other:
            to["gz"] = 2 * chip + (1 - core)
        return to

    def along(step):
        to = lax.rem(chip + step, chips)
        return dict(device(), gz=2 * to + core), to > chip

    def hops(step):
        sizes_here = (NX, NY, 2) if len(step) == 3 else (chips,)
        return -sum(min(v, n - v) for v, n in zip(step, sizes_here))

    steps = sorted(itertools.product(range(NX), range(NY), range(2)), key=hops)
    plane_peers = [in_plane(*step) for step in steps if any(step)]
    line_peers = [along(*step) for step in sorted([(k,) for k in range(1, chips)], key=hops)]
    across = 2 * core - 1
    next_peers = [
        dict(device(dy=dy), gz=lax.rem(gz + across + NZ, NZ)) for dy in (-1, 0, 1)
    ]
    bottom, top = gz == 0, gz == NZ - 1
    barrier = pltpu.get_barrier_semaphore()

    def greet(semaphore, peer):
        pl.semaphore_signal(semaphore, inc=1, device_id=peer, device_id_type=MESH)

    def wait(semaphore, amount):
        pl.when(amount > 0)(functools.partial(pl.semaphore_wait, semaphore, amount))

    chunks = load_sem.shape[0]
    depth = nz // chunks
    loads = []
    for c in range(chunks):
        copy = pltpu.make_async_copy(
            res.at[:, pl.ds(c * depth, depth)],
            R.at[:, pl.ds(HALO + c * depth, depth), pl.ds(0, ny)],
            load_sem.at[c],
        )
        copy.start()
        loads.append(copy)
    dens_copy = pltpu.make_async_copy(dens, D, dens_sem)
    dens_copy.start()

    for peer, above in line_peers:
        pl.when(above)(functools.partial(greet, barrier, peer))
    for peer in plane_peers:
        greet(barrier, peer)

    @pl.when(jnp.logical_not(top))
    def _():
        for peer in next_peers:
            greet(barrier, peer)

    main = pl.ds(HALO, nz)
    inner = pl.ds(0, ny)
    end_z = HALO + nz
    moves = [
        (res.at[:, :, pl.ds(0, 3)], R.at[:, main, pl.ds(ny, 3)], device(dy=-1)),
        (res.at[:, :, pl.ds(ny - 3, 3)], R.at[:, main, pl.ds(ring - 3, 3)], device(dy=1)),
        (res.at[:, pl.ds(0, 3)], R.at[:, pl.ds(end_z, 3), inner], device(dz=-1)),
        (res.at[:, pl.ds(nz - 3, 3)], R.at[:, pl.ds(0, 3), inner], device(dz=1)),
    ]
    for sy, sz in itertools.product((-1, 1), (-1, 1)):
        zs, zd = (0, end_z) if sz < 0 else (nz - 2, 1)
        ys, yd = (0, ny) if sy < 0 else (ny - 2, ring - 2)
        moves.append((
            res.at[:, pl.ds(zs, 2), pl.ds(ys, 2)],
            R.at[:, pl.ds(zd, 2), pl.ds(yd, 2)],
            device(dy=sy, dz=sz),
        ))
    bulk = [
        pltpu.make_async_remote_copy(
            src, dst, bulk_send, bulk_recv.at[0 if k in (2, 3) else 1],
            device_id=peer, device_id_type=MESH,
        )
        for k, (src, dst, peer) in enumerate(moves)
    ]
    def plane_products(z, sums):
        sums = list(sums)
        for t in range(ny // 8):
            rows = [R[i, HALO + z, 8 * t : 8 * t + 8, :] for i in range(HIST)]
            for k, (i, j) in enumerate(PAIRS):
                sums[k] = sums[k] + rows[i] * rows[j]
        return tuple(sums)

    sums = tuple(jnp.zeros((8, 128), jnp.float32) for _ in PAIRS)
    for c in range(chunks):
        loads[c].wait()
        sums = lax.fori_loop(c * depth, (c + 1) * depth, plane_products, sums)
    lane = lanes((8, 128))
    partial = jnp.zeros((8, 128), jnp.float32)
    for k in range(len(PAIRS)):
        partial = jnp.where(lane == k, jnp.sum(sums[k], axis=1, keepdims=True), partial)
    row = jnp.sum(partial, axis=0, keepdims=True)

    def share(buf, slot, value, peers, phase):
        buf[slot] = value
        for peer in peers:
            pltpu.make_async_remote_copy(
                buf.at[slot], buf.at[slot], gram_send.at[phase], gram_recv.at[phase],
                device_id=peer, device_id_type=MESH,
            ).start()
        return buf.at[pl.ds(0, len(peers))]

    def summed(buf, others, phase):
        pltpu.make_async_copy(others, others, gram_recv.at[phase]).wait()
        total = buf[0]
        for k in range(1, buf.shape[0]):
            total = total + buf[k]
        return total

    few = len(next_peers)
    pl.semaphore_wait(barrier, len(plane_peers) + chip + few - few * bottom.astype(jnp.int32))
    others1 = share(G1, (gx * NY + gy) * 2 + core, row, plane_peers, 0)
    for peer, above in line_peers:
        pl.when(jnp.logical_not(above))(functools.partial(greet, entered.at[1], peer))

    @pl.when(top)
    def _():
        for peer in next_peers:
            greet(entered.at[0], peer)

    over = [bottom if k in (2, 4, 6) else None for k in range(len(bulk))]
    for copy, late in zip(bulk, over):
        if late is None:
            copy.start()
        else:
            pl.when(jnp.logical_not(late))(copy.start)

    @pl.when(bottom)
    def _():
        pl.semaphore_wait(entered.at[0], few)
        for k in (2, 4, 6):
            bulk[k].start()

    plane_row = summed(G1, others1, 0)
    wait(entered.at[1], chips - 1 - chip)
    others2 = share(G2, chip, plane_row, [peer for peer, _ in line_peers], 1)

    def arrived(semaphore, rows):
        width = ring if rows % ring == 0 else 8
        view = R.at[:, pl.ds(0, rows // width), pl.ds(0, width)]
        pltpu.make_async_copy(view, view, semaphore).wait()

    def pack_rows(low, high, i, _):
        wide = lanes((high - low, 128))
        for v in range((ZR + 1) // 2):
            part = jnp.zeros((high - low, 128), jnp.float32)
            for zr in range(2 * v, min(2 * v + 2, ZR)):
                for p in range(zr, nz + 4, ZR):
                    base = (p // ZR) * SLOT + 2 * HALO * (zr - 2 * v)
                    here = (wide >= base) & (wide < base + 2 * HALO)
                    moved = pltpu.roll(R[i, p + 1, low:high], (base + HALO) % 128, 1)
                    part = jnp.where(here, moved, part)
            packs[i, v, low:high] = part

    arrived(bulk_recv.at[0], 2 * HALO * ny)
    lax.fori_loop(0, HIST, functools.partial(pack_rows, 0, ny), None)
    arrived(bulk_recv.at[1], 2 * HALO * nz + 16)
    for i in range(HIST):
        pack_rows(ny, ring, i, None)
    wide = lanes((ring, 128))
    arrived(bulk_send, 2 * HALO * (nz + ny) + 16)
    pltpu.make_async_copy(others1, others1, gram_send.at[0]).wait()

    total = summed(G2, others2, 1)
    shares = pulay(total)
    for i in range(HIST):
        weights[i] = shares[i]
    shares = [weights[i] for i in range(HIST)]
    tiles = ring // 8

    def weighted(entries):
        out = None
        for share_i, entry in zip(shares, entries):
            term = share_i[None] * entry.reshape(-1, 8, 128)
            out = term if out is None else out + term
        return out.reshape(-1, 128)

    parts = [weighted([packs[i, v] for i in range(HIST)]) for v in range((ZR + 1) // 2)]
    place = wide % SLOT
    for side, own in enumerate((own_right, own_left)):
        edge = jnp.zeros((ring, 128), jnp.float32)
        for zr in range(ZR):
            source = 2 * HALO * (zr % 2) + HALO * side
            moved = pltpu.roll(parts[zr // 2], (HALO * zr - source) % 128, 1)
            edge = jnp.where((place >= HALO * zr) & (place < HALO * (zr + 1)), moved, edge)
        own[...] = edge
    for own, there, dx in ((own_left, from_right, -1), (own_right, from_left, 1)):
        pltpu.make_async_remote_copy(
            own, there, edge_send, edge_recv, device_id=device(dx=dx), device_id_type=MESH
        ).start()

    def combine(k, _):
        C[k] = weighted([R[i, k] for i in range(HIST)])

    unrolled(nz + 2 * HALO, (nz + 2 * HALO) // 2, combine)

    def around(v, rows=ring):
        total = (pltpu.roll(v, 1, 0) + pltpu.roll(v, ring - 1, 0))[:rows]
        v = v[:rows]
        return total + pltpu.roll(v, 1, 1) + pltpu.roll(v, 127, 1)

    def sweep1(k, _):
        v = C[k + 1]
        T1[k] = 6.0 * v - (C[k] + C[k + 2] + around(v))

    def sweep2(k, _):
        v = T1[k + 1]
        T2[k] = A2 * v + B2 * (T1[k] + T1[k + 2] + around(v))

    def sweep3(k, _):
        v = T2[k + 1]
        near_z = T1[k + 2, :ny] + T2[k, :ny] + T2[k + 2, :ny]
        out = K1 * v[:ny] + K2 * (near_z + around(v, ny))
        acc[k] = out + weighted([D[i, k] for i in range(HIST)])

    unrolled(nz + 4, 18, sweep1)
    unrolled(nz + 2, (nz + 2) // 2, sweep2)
    dens_copy.wait()
    unrolled(nz, 16, sweep3)
    both = C.at[pl.ds(0, 2)]
    pltpu.make_async_copy(both, both, edge_recv).wait()
    pltpu.make_async_copy(both, both, edge_send).wait()
    pltpu.make_async_copy(others2, others2, gram_send.at[1]).wait()


def finish(acc, from_left, from_right, own_left, own_right, weights, out, coeffs,
           buf, row_buf, sem, row_sem):
    nz, ny = acc.shape[0], acc.shape[1]
    coeff_lane = lanes((1, 128))
    row = jnp.zeros((1, 128), jnp.float32)
    for i in range(HIST):
        row = jnp.where(coeff_lane == i, weights[i, 0:1, :], row)
    row_buf[...] = row[:, :HIST]
    row_copy = pltpu.make_async_copy(row_buf, coeffs, row_sem)
    row_copy.start()

    beyond = spread(from_left[...] - own_right[...], from_right[...] - own_left[...])
    change = [v[:ny] for v in relaxed(beyond)]
    lane = lanes((ny, 128))
    near, far = lane < HALO, lane >= 128 - HALO
    chunks = sem.shape[0]
    copies = []
    for z in range(nz):
        zq, zr = divmod(z + 2, ZR)
        at_left = pltpu.roll(change[zr], (-(SLOT * zq + HALO)) % 128, 1)
        at_right = pltpu.roll(change[zr], (125 - (SLOT * zq + 2 * HALO)) % 128, 1)
        buf[z] = acc[z] + jnp.where(near, at_left, jnp.where(far, at_right, 0.0))
        depth = nz // chunks
        if z % depth == depth - 1:
            c = z // depth
            part = pl.ds(c * depth, depth)
            copy = pltpu.make_async_copy(buf.at[part], out.at[part], sem.at[c])
            copy.start()
            copies.append(copy)
    for copy in copies:
        copy.wait()
    row_copy.wait()


def on_device(sizes, densities, residuals):
    _, nz, ny, nx = residuals.shape
    ring, deep = ny + 8, nz + 2 * HALO
    f32 = jnp.float32
    vmem, hbm = pl.BlockSpec(memory_space=pltpu.VMEM), pl.BlockSpec(memory_space=pltpu.HBM)
    edge = pltpu.VMEM((ring, nx), f32)
    NX, NY, NZ = sizes
    dma = pltpu.SemaphoreType.DMA
    middle = pl.pallas_call(
        functools.partial(exchange, sizes),
        out_shape=(
            pltpu.VMEM((nz, ny, nx), f32), edge, edge, edge, edge,
            pltpu.VMEM((HIST, 8, 128), f32),
        ),
        in_specs=[hbm, hbm],
        out_specs=(vmem,) * 6,
        scratch_shapes=[
            pltpu.VMEM((HIST, deep, ring, nx), f32),
            pltpu.VMEM((HIST, nz, ny, nx), f32),
            pltpu.VMEM((deep, ring, nx), f32),
            pltpu.VMEM((deep - 2, ring, nx), f32),
            pltpu.VMEM((deep - 4, ring, nx), f32),
            pltpu.VMEM((NX * NY * 2, 1, 128), f32),
            pltpu.VMEM((NZ // 2, 1, 128), f32),
            pltpu.VMEM((HIST, (ZR + 1) // 2, ring, nx), f32),
            dma((8,)), dma(()), dma(()), dma((2,)), dma(()), dma(()), dma((2,)), dma((2,)),
            pltpu.SemaphoreType.REGULAR((2,)),
        ],
        compiler_params=pltpu.CompilerParams(
            collective_id=0, has_side_effects=True, vmem_limit_bytes=60 << 20
        ),
    )(densities, residuals)
    density, coeffs = pl.pallas_call(
        finish,
        out_shape=(
            jax.ShapeDtypeStruct((nz, ny, nx), f32),
            jax.ShapeDtypeStruct((1, HIST), f32),
        ),
        in_specs=[vmem] * 6,
        out_specs=(hbm, hbm),
        scratch_shapes=[
            pltpu.VMEM((nz, ny, nx), f32), pltpu.VMEM((1, HIST), f32), dma((4,)), dma(()),
        ],
        compiler_params=pltpu.CompilerParams(vmem_limit_bytes=16 << 20),
    )(*middle)
    return density, coeffs.reshape(HIST)


def solution(mesh):
    sizes = tuple(mesh.shape[a] for a in ("gx", "gy", "gz"))
    spec = P(None, "gz", "gy", "gx")
    return jax.shard_map(
        functools.partial(on_device, sizes),
        mesh=mesh,
        in_specs=(spec, spec),
        out_specs=(P("gz", "gy", "gx"), P()),
        check_vma=False,
    )
```
